32 devices in a mesh: shot: 4 (over x, core), tile: 8 (over z, y).
Axes of the slice: x: 2, y: 2, z: 4, core: 2. Of those that a mesh axis runs over, the one named last changes fastest.
Arguments:
- partials: bfloat16 [32, 8, 512, 512], P(('shot', 'tile')), may hold values from -6 to 6
Outputs:
- filtered: float32 [8, 512, 512], P('shot', 'tile')
The draws below stay inside these ranges and needn't reach their ends.
All inputs are finite; a program needn't handle non-finite values.
Results may differ from the reference program's by a relative error of at most 0.0003.
Values may be sent and summed in bfloat16 or wider, within the bound.
A program may use at most 64 MiB of HBM per device.

```python
import jax
import jax.numpy as jnp
from jax import lax

DEPTH = 8
NX = 512
NY = 512
SHOTS = 32


def block_scale(key, shape, shards, low, high):
    level = 1.0
    for dim, blocks in shards:
        draws = jax.random.uniform(jax.random.fold_in(jax.random.fold_in(key, 6), dim), (blocks,), jnp.float32, low / len(shards), high / len(shards))
        level = level * jnp.repeat(jnp.exp(draws), shape[dim] // blocks).reshape((-1,) + (1,) * (len(shape) - 1 - dim))
    return level


def gaussian(own_key, extent, spread, bound, pieces=(), kind=jnp.bfloat16):
    result = jax.random.normal(own_key, extent, jnp.float32) * spread
    if len(pieces) > 0:
        result = block_scale(own_key, extent, pieces, -0.22, 0.18) * result
    return jnp.clip(result, min=-bound, max=bound).astype(kind)


def setup_inputs(seed: int = 0) -> dict:
    splits = jax.random.split(jax.random.key(seed), 2)
    return {
        "partials": gaussian(splits[0], (SHOTS, DEPTH, NX, NY), 1.0, 6.0, ((0, 32),)),
    }


def reference(partials):

    def add_one(total, piece):
        return (total + piece.astype(jnp.float32), None)
    start = jnp.zeros((DEPTH, NX, NY), jnp.float32)
    stack, unused = lax.scan(add_one, start, partials)
    image = stack / jnp.sqrt(jnp.float32(SHOTS))
    padded = jnp.pad(image, 1)
    beside = padded[2:, 1:-1, 1:-1] + padded[:-2, 1:-1, 1:-1]
    beside = beside + padded[1:-1, 2:, 1:-1] + padded[1:-1, :-2, 1:-1]
    beside = beside + padded[1:-1, 1:-1, 2:] + padded[1:-1, 1:-1, :-2]
    return 6.0 * image - beside
```

```python
import functools

import jax
import jax.numpy as jnp
from jax import lax
from jax.experimental import pallas as pl
from jax.experimental.pallas import tpu as pltpu
from jax.sharding import PartitionSpec as P

MESH = pl.DeviceIdType.MESH
F32 = jnp.float32


def kernel(groups, members, src, out, own_a, own_b, r1a, r1b, s1a, s1b, r2a, r2b,
           s2, r3, s3, r4, img, low, high, top, bottom, own_sem,
           p1s, p1r, q1s, q1r, p2s, p2r, p3s, p3r, hs, hr):
    nd, nz, rows, width = src.shape[2], src.shape[3], src.shape[5], src.shape[6]
    cw = width // 4
    edge = top.shape[1]
    steps = 2 * nd
    g, t = lax.axis_index("shot"), lax.axis_index("tile")
    x, c = g // 2, g % 2
    z, y = t // 2, t % 2

    def dev(gx, tx):
        return {"shot": gx, "tile": tx}

    x_peer = dev((1 - x) * 2 + c, t)
    c_peer = dev(x * 2 + 1 - c, t)
    y_peer = dev(g, z * 2 + 1 - y)

    def z_peer(o):
        return dev(g, lax.rem(z + o, nz) * 2 + y)

    beside = [
        (g > 0, dev(g - 1, t)),
        (g < groups - 1, dev(g + 1, t)),
        (t > 0, dev(g, t - 1)),
        (t < members - 1, dev(g, t + 1)),
    ]

    loads = [
        pltpu.make_async_copy(src.at[x, :, :, :, :, :, pl.ds(0, 2 * cw)], own_a, own_sem.at[0]),
        pltpu.make_async_copy(src.at[:, :, :, :, y, :, pl.ds(2 * cw, 2 * cw)], own_b, own_sem.at[1]),
    ]
    for copy in loads:
        copy.start()

    barrier = pltpu.get_barrier_semaphore()
    peers = [x_peer, c_peer, y_peer] + [z_peer(o) for o in range(1, nz)]
    count = jnp.int32(len(peers))
    for peer in peers:
        pl.semaphore_signal(barrier, inc=1, device_id=peer, device_id_type=MESH)
    for there, peer in beside:
        count = count + jnp.where(there, 1, 0)

        @pl.when(there)
        def _():
            pl.semaphore_signal(barrier, inc=1, device_id=peer, device_id_type=MESH)
    pl.semaphore_wait(barrier, count)

    sends = []

    def remote(a, b, s, r, peer):
        copy = pltpu.make_async_remote_copy(
            src_ref=a, dst_ref=b, send_sem=s, recv_sem=r, device_id=peer, device_id_type=MESH
        )
        copy.start()
        sends.append(copy)
        return copy

    first, second, third, fourth = {}, {}, {}, {}

    def p1(k):
        block, d = k // nd, k % nd
        first[k] = (
            remote(src.at[1 - x, :, d, :, :, :, pl.ds(block * cw, cw)], r1a.at[k],
                   p1s.at[0, k], p1r.at[0, k], x_peer),
            remote(src.at[:, :, d, :, 1 - y, :, pl.ds((2 + block) * cw, cw)], r1b.at[k],
                   p1s.at[1, k], p1r.at[1, k], y_peer),
        )

    def two_a(k, core, side):
        block, d = k // nd, k % nd
        own = own_a[core, d, :, side, :, pl.ds(block * cw, cw)]
        return own.astype(F32) + r1a[k, core, :, side].astype(F32)

    def two_b(k, core, side):
        block, d = k // nd, k % nd
        own = own_b[side, core, d, :, :, pl.ds(block * cw, cw)]
        return own.astype(F32) + r1b[k, side, core].astype(F32)

    def q1(k):
        a, b = first[k]
        a.wait_recv()
        for side in range(2):
            s1a[k, side] = two_a(k, 1 - c, side)
        ca = remote(s1a.at[k], r2a.at[k], q1s.at[0, k], q1r.at[0, k], c_peer)
        b.wait_recv()
        for side in range(2):
            s1b[k, side] = two_b(k, 1 - c, side)
        cb = remote(s1b.at[k], r2b.at[k], q1s.at[1, k], q1r.at[1, k], c_peer)
        second[k] = (ca, cb)

    def p2(k):
        a, b = second[k]
        a.wait_recv()
        s2[0, k] = two_a(k, c, 1 - y) + r2a[k, 1 - y]
        ca = remote(s2.at[0, k], r3.at[0, k], p2s.at[0, k], p2r.at[0, k], y_peer)
        b.wait_recv()
        s2[1, k] = two_b(k, c, 1 - x) + r2b[k, 1 - x]
        cb = remote(s2.at[1, k], r3.at[1, k], p2s.at[1, k], p2r.at[1, k], x_peer)
        third[k] = (ca, cb)

    def p3(k):
        copies = []
        for kind in range(2):
            third[k][kind].wait_recv()
            if kind == 0:
                s3[0, k] = two_a(k, c, y) + r2a[k, y] + r3[0, k]
            else:
                s3[1, k] = two_b(k, c, x) + r2b[k, x] + r3[1, k]
            for o in range(1, nz):
                to = lax.rem(z + o, nz)
                copies.append(remote(s3.at[kind, k, to], r4.at[kind, k, z],
                                     p3s.at[kind, k, o - 1], p3r.at[kind, k, o - 1], z_peer(o)))
        fourth[k] = copies

    scale = 1.0 / jnp.sqrt(F32(groups * members))
    halo_waits = []

    def halo(there_to, peer_to, there_from, peer_from, a, b, s, r):
        def make(peer):
            return pltpu.make_async_remote_copy(
                src_ref=a, dst_ref=b, send_sem=s, recv_sem=r, device_id=peer, device_id_type=MESH
            )

        @pl.when(there_to)
        def _():
            make(peer_to).start()

        def done():
            @pl.when(there_from)
            def _():
                make(peer_from).wait_recv()

            @pl.when(there_to)
            def _():
                make(peer_to).wait_send()

        halo_waits.append(done)

    def last(k):
        block, d = k // nd, k % nd
        for kind in range(2):
            cols = pl.ds((2 * kind + block) * cw, cw)
            total = s3[kind, k, z]
            for o in range(1, nz):
                fourth[k][kind * (nz - 1) + o - 1].wait_recv()
                total = total + r4[kind, k, lax.rem(z + nz - o, nz)]
            img[d, :, cols] = total * scale
            if d == 0:
                halo(*beside[0], *beside[1], img.at[d, :, cols], high.at[:, cols], hs.at[0, kind, k], hr.at[0, kind, k])
            if d == nd - 1:
                halo(*beside[1], *beside[0], img.at[d, :, cols], low.at[:, cols], hs.at[1, kind, k], hr.at[1, kind, k])
            halo(*beside[2], *beside[3], img.at[d, pl.ds(0, edge), cols], bottom.at[d, :, cols],
                 hs.at[2, kind, k], hr.at[2, kind, k])
            halo(*beside[3], *beside[2], img.at[d, pl.ds(rows - edge, edge), cols], top.at[d, :, cols],
                 hs.at[3, kind, k], hr.at[3, kind, k])

    p1(0)
    p1(1)
    for copy in loads:
        copy.wait()
    for k in range(steps):
        q1(k)
        p2(k)
        if k + 2 < steps:
            p1(k + 2)
        if k >= 1:
            p3(k - 1)
        if k >= 2:
            last(k - 2)
    last(steps - 2)
    p3(steps - 1)
    last(steps - 1)
    for done in halo_waits:
        done()

    row = lax.broadcasted_iota(jnp.int32, (rows, width), 0)
    col = lax.broadcasted_iota(jnp.int32, (rows, width), 1)
    for d in range(nd):
        here = img[d]
        below = img[d - 1] if d > 0 else jnp.where(g > 0, low[...], 0.0)
        above = img[d + 1] if d < nd - 1 else jnp.where(g < groups - 1, high[...], 0.0)
        before = jnp.where(t > 0, top[d, edge - 1:edge, :], 0.0)
        after = jnp.where(t < members - 1, bottom[d, 0:1, :], 0.0)
        near = above + below
        near = near + jnp.where(row == rows - 1, after, pltpu.roll(here, rows - 1, 0))
        near = near + jnp.where(row == 0, before, pltpu.roll(here, 1, 0))
        near = near + jnp.where(col == width - 1, 0.0, pltpu.roll(here, width - 1, 1))
        near = near + jnp.where(col == 0, 0.0, pltpu.roll(here, 1, 1))
        out[d] = 6.0 * here - near
    for copy in sends:
        copy.wait_send()


def body(groups, members, partials):
    shots, depth, lateral, width = partials.shape
    nd, nz, rows, cw = depth // groups, members // 2, lateral // members, width // 4
    steps, edge = 2 * nd, min(8, rows)
    src = partials.reshape(2, 2, nd, nz, 2, rows, width)
    kind = partials.dtype
    dma = pltpu.SemaphoreType.DMA
    return pl.pallas_call(
        functools.partial(kernel, groups, members),
        out_shape=jax.ShapeDtypeStruct((nd, rows, width), F32),
        in_specs=[pl.BlockSpec(memory_space=pl.ANY)],
        out_specs=pl.BlockSpec(memory_space=pltpu.VMEM),
        scratch_shapes=[
            pltpu.VMEM((2, nd, nz, 2, rows, 2 * cw), kind),
            pltpu.VMEM((2, 2, nd, nz, rows, 2 * cw), kind),
            pltpu.VMEM((steps, 2, nz, 2, rows, cw), kind),
            pltpu.VMEM((steps, 2, 2, nz, rows, cw), kind),
            pltpu.VMEM((steps, 2, nz, rows, cw), F32),
            pltpu.VMEM((steps, 2, nz, rows, cw), F32),
            pltpu.VMEM((steps, 2, nz, rows, cw), F32),
            pltpu.VMEM((steps, 2, nz, rows, cw), F32),
            pltpu.VMEM((2, steps, nz, rows, cw), F32),
            pltpu.VMEM((2, steps, nz, rows, cw), F32),
            pltpu.VMEM((2, steps, nz, rows, cw), F32),
            pltpu.VMEM((2, steps, nz, rows, cw), F32),
            pltpu.VMEM((nd, rows, width), F32),
            pltpu.VMEM((rows, width), F32),
            pltpu.VMEM((rows, width), F32),
            pltpu.VMEM((nd, edge, width), F32),
            pltpu.VMEM((nd, edge, width), F32),
            dma((2,)),
            dma((2, steps)), dma((2, steps)),
            dma((2, steps)), dma((2, steps)),
            dma((2, steps)), dma((2, steps)),
            dma((2, steps, nz - 1)), dma((2, steps, nz - 1)),
            dma((4, 2, steps)), dma((4, 2, steps)),
        ],
        compiler_params=pltpu.CompilerParams(collective_id=0, has_side_effects=True),
    )(src)


def solution(mesh):
    groups, members = mesh.shape["shot"], mesh.shape["tile"]
    return jax.shard_map(
        functools.partial(body, groups, members),
        mesh=mesh,
        in_specs=(P(("shot", "tile"), None, None, None),),
        out_specs=P("shot", "tile", None),
        check_vma=False,
    )
```

```python
import functools

import jax
import jax.numpy as jnp
from jax import lax
from jax.experimental import pallas as pl
from jax.experimental.pallas import tpu as pltpu
from jax.sharding import PartitionSpec as P

MESH = pl.DeviceIdType.MESH
F32 = jnp.float32


def kernel(groups, members, src, out, own_a, own_b, own_c, r1a, r1b, s1a, s1b, r2a, r2b,
           s2, r3, s3, r4, rz, sc, rc, tc, rd, img, low, high, top, bottom, own_sem,
           p1s, p1r, q1s, q1r, p2s, p2r, p3s, p3r, zs, zr, cs, cr, ds, dr, hs, hr):
    nd, nz, rows, width = src.shape[2], src.shape[3], src.shape[5], src.shape[6]
    cw = width // 4
    rr = s2.shape[3]
    parts = rows // rr
    edge = top.shape[1]
    units = [(j, d, h) for j in range(2) for d in range(nd) for h in range(parts)]
    cj, cd, ch = units.pop()
    steps = len(units)
    g, t = lax.axis_index("shot"), lax.axis_index("tile")
    x, c = g // 2, g % 2
    z, y = t // 2, t % 2

    def dev(gx, tx):
        return {"shot": gx, "tile": tx}

    x_peer = dev((1 - x) * 2 + c, t)
    c_peer = dev(x * 2 + 1 - c, t)
    y_peer = dev(g, z * 2 + 1 - y)
    d_peer = dev((1 - x) * 2 + c, z * 2 + 1 - y)

    def z_peer(o):
        return dev(g, lax.rem(z + o, nz) * 2 + y)

    beside = [
        (g > 0, dev(g - 1, t)),
        (g < groups - 1, dev(g + 1, t)),
        (t > 0, dev(g, t - 1)),
        (t < members - 1, dev(g, t + 1)),
    ]

    def col(kind, j):
        return pl.ds((2 * kind + j) * cw, cw)

    def row(h):
        return pl.ds(h * rr, rr)

    barrier = pltpu.get_barrier_semaphore()
    peers = [x_peer, c_peer, y_peer, d_peer] + [z_peer(o) for o in range(1, nz)]
    count = jnp.int32(len(peers))
    for peer in peers:
        pl.semaphore_signal(barrier, inc=1, device_id=peer, device_id_type=MESH)
    for there, peer in beside:
        count = count + jnp.where(there, 1, 0)

        @pl.when(there)
        def _():
            pl.semaphore_signal(barrier, inc=1, device_id=peer, device_id_type=MESH)
    loads = [
        pltpu.make_async_copy(src.at[x, :, :, :, :, :, pl.ds(0, 2 * cw)], own_a, own_sem.at[0]),
        pltpu.make_async_copy(src.at[:, :, :, :, y, :, pl.ds(2 * cw, 2 * cw)], own_b, own_sem.at[1]),
    ]
    for kind in range(2):
        loads.append(pltpu.make_async_copy(src.at[:, :, cd, z, :, row(ch), col(kind, cj)],
                                           own_c.at[kind], own_sem.at[2 + kind]))
    for copy in loads:
        copy.start()
    pl.semaphore_wait(barrier, count)

    sends = []

    def remote(a, b, s, r, peer):
        copy = pltpu.make_async_remote_copy(
            src_ref=a, dst_ref=b, send_sem=s, recv_sem=r, device_id=peer, device_id_type=MESH
        )
        copy.start()
        sends.append(copy)
        return copy

    first, second, third, fourth = {}, {}, {}, {}

    def p1(k):
        j, d, h = units[k]
        first[k] = (
            remote(src.at[1 - x, :, d, :, :, row(h), col(0, j)], r1a.at[k],
                   p1s.at[0, k], p1r.at[0, k], x_peer),
            remote(src.at[:, :, d, :, 1 - y, row(h), col(1, j)], r1b.at[k],
                   p1s.at[1, k], p1r.at[1, k], y_peer),
        )

    def two_a(k, core, side):
        j, d, h = units[k]
        own = own_a[core, d, :, side, row(h), pl.ds(j * cw, cw)]
        return own.astype(F32) + r1a[k, core, :, side].astype(F32)

    def two_b(k, core, side):
        j, d, h = units[k]
        own = own_b[side, core, d, :, row(h), pl.ds(j * cw, cw)]
        return own.astype(F32) + r1b[k, side, core].astype(F32)

    def q1(k):
        a, b = first[k]
        a.wait_recv()
        for side in range(2):
            s1a[k, side] = two_a(k, 1 - c, side)
        ca = remote(s1a.at[k], r2a.at[k], q1s.at[0, k], q1r.at[0, k], c_peer)
        b.wait_recv()
        for side in range(2):
            s1b[k, side] = two_b(k, 1 - c, side)
        cb = remote(s1b.at[k], r2b.at[k], q1s.at[1, k], q1r.at[1, k], c_peer)
        second[k] = (ca, cb)

    def p2(k):
        a, b = second[k]
        a.wait_recv()
        s2[0, k] = two_a(k, c, 1 - y) + r2a[k, 1 - y]
        ca = remote(s2.at[0, k], r3.at[0, k], p2s.at[0, k], p2r.at[0, k], y_peer)
        b.wait_recv()
        s2[1, k] = two_b(k, c, 1 - x) + r2b[k, 1 - x]
        cb = remote(s2.at[1, k], r3.at[1, k], p2s.at[1, k], p2r.at[1, k], x_peer)
        third[k] = (ca, cb)

    def p3(k):
        copies = []
        for kind in range(2):
            third[k][kind].wait_recv()
            if kind == 0:
                s3[0, k] = two_a(k, c, y) + r2a[k, y] + r3[0, k]
            else:
                s3[1, k] = two_b(k, c, x) + r2b[k, x] + r3[1, k]
            for o in range(1, nz):
                to = lax.rem(z + o, nz)
                copies.append(remote(s3.at[kind, k, to], r4.at[kind, k, z],
                                     p3s.at[kind, k, o - 1], p3r.at[kind, k, o - 1], z_peer(o)))
        fourth[k] = copies

    z_first, z_core, z_last = [], [], []

    def c_z():
        for kind in range(2):
            for o in range(1, nz):
                to = lax.rem(z + o, nz)
                z_first.append(remote(src.at[:, :, cd, to, :, row(ch), col(kind, cj)], rz.at[kind, o - 1],
                                      zs.at[kind, o - 1], zr.at[kind, o - 1], z_peer(o)))

    def c_sum(kind, core, side):
        total = own_c[kind, side, core].astype(F32)
        for o in range(1, nz):
            total = total + rz[kind, o - 1, side, core].astype(F32)
        return total

    def c_core():
        for kind in range(2):
            for o in range(1, nz):
                z_first[kind * (nz - 1) + o - 1].wait_recv()
            for side in range(2):
                sc[kind, side] = c_sum(kind, 1 - c, side)
            z_core.append(remote(sc.at[kind], rc.at[kind], cs.at[kind], cr.at[kind], c_peer))

    def c_xy():
        for kind in range(2):
            z_core[kind].wait_recv()
            for side in range(2):
                tc[kind, side] = c_sum(kind, c, side) + rc[kind, side]
            for i, (a, b, peer) in enumerate(
                [(1 - x, 1 - y, d_peer), (1 - x, y, x_peer), (x, 1 - y, y_peer)]
            ):
                z_last.append(remote(tc.at[kind, a, b], rd.at[kind, i], ds.at[kind, i], dr.at[kind, i], peer))

    scale = 1.0 / jnp.sqrt(F32(groups * members))
    halo_waits = []

    def halo(there_to, peer_to, there_from, peer_from, a, b, s, r):
        def make(peer):
            return pltpu.make_async_remote_copy(
                src_ref=a, dst_ref=b, send_sem=s, recv_sem=r, device_id=peer, device_id_type=MESH
            )

        @pl.when(there_to)
        def _():
            make(peer_to).start()

        def done():
            @pl.when(there_from)
            def _():
                make(peer_from).wait_recv()

            @pl.when(there_to)
            def _():
                make(peer_to).wait_send()

        halo_waits.append(done)

    def finish(kind, unit, k, total):
        j, d, h = unit
        cols = col(kind, j)
        img[d, row(h), cols] = total * scale
        if d == 0:
            halo(*beside[0], *beside[1], img.at[d, row(h), cols], high.at[row(h), cols],
                 hs.at[0, kind, k], hr.at[0, kind, k])
        if d == nd - 1:
            halo(*beside[1], *beside[0], img.at[d, row(h), cols], low.at[row(h), cols],
                 hs.at[1, kind, k], hr.at[1, kind, k])
        if h == 0:
            halo(*beside[2], *beside[3], img.at[d, pl.ds(0, edge), cols], bottom.at[d, :, cols],
                 hs.at[2, kind, k], hr.at[2, kind, k])
        if h == parts - 1:
            halo(*beside[3], *beside[2], img.at[d, pl.ds(rows - edge, edge), cols], top.at[d, :, cols],
                 hs.at[3, kind, k], hr.at[3, kind, k])

    def last(k):
        for kind in range(2):
            total = s3[kind, k, z]
            for o in range(1, nz):
                fourth[k][kind * (nz - 1) + o - 1].wait_recv()
                total = total + r4[kind, k, lax.rem(z + nz - o, nz)]
            finish(kind, units[k], k, total)

    def c_last():
        for kind in range(2):
            total = tc[kind, x, y]
            for i in range(3):
                z_last[kind * 3 + i].wait_recv()
                total = total + rd[kind, i]
            finish(kind, (cj, cd, ch), steps, total)

    at_core = min(3, steps - 1)
    at_xy = max(steps - 2, at_core)
    ahead = 3
    p1(0)
    c_z()
    for k in range(1, min(ahead, steps)):
        p1(k)
    for copy in loads:
        copy.wait()
    for k in range(steps):
        q1(k)
        p2(k)
        if k + ahead < steps:
            p1(k + ahead)
        if k >= 2:
            p3(k - 2)
        if k == at_core:
            c_core()
        if k == at_xy:
            c_xy()
        if k >= 4:
            last(k - 4)
    for k in range(max(steps - 2, 0), steps):
        p3(k)
    for k in range(max(steps - 4, 0), steps - 1):
        last(k)
    c_last()
    last(steps - 1)
    for done in halo_waits:
        done()

    rown = lax.broadcasted_iota(jnp.int32, (rows, width), 0)
    coln = lax.broadcasted_iota(jnp.int32, (rows, width), 1)
    for d in range(nd):
        here = img[d]
        below = img[d - 1] if d > 0 else jnp.where(g > 0, low[...], 0.0)
        above = img[d + 1] if d < nd - 1 else jnp.where(g < groups - 1, high[...], 0.0)
        before = jnp.where(t > 0, top[d, edge - 1:edge, :], 0.0)
        after = jnp.where(t < members - 1, bottom[d, 0:1, :], 0.0)
        near = above + below
        near = near + jnp.where(rown == rows - 1, after, pltpu.roll(here, rows - 1, 0))
        near = near + jnp.where(rown == 0, before, pltpu.roll(here, 1, 0))
        near = near + jnp.where(coln == width - 1, 0.0, pltpu.roll(here, width - 1, 1))
        near = near + jnp.where(coln == 0, 0.0, pltpu.roll(here, 1, 1))
        out[d] = 6.0 * here - near
    for copy in sends:
        copy.wait_send()


def body(groups, members, partials):
    shots, depth, lateral, width = partials.shape
    nd, nz, rows, cw = depth // groups, members // 2, lateral // members, width // 4
    parts = 2 if rows % 32 == 0 else 1
    rr, edge = rows // parts, min(8, rows)
    steps = 2 * nd * parts - 1
    src = partials.reshape(2, 2, nd, nz, 2, rows, width)
    kind = partials.dtype
    dma = pltpu.SemaphoreType.DMA
    return pl.pallas_call(
        functools.partial(kernel, groups, members),
        out_shape=jax.ShapeDtypeStruct((nd, rows, width), F32),
        in_specs=[pl.BlockSpec(memory_space=pl.ANY)],
        out_specs=pl.BlockSpec(memory_space=pltpu.VMEM),
        scratch_shapes=[
            pltpu.VMEM((2, nd, nz, 2, rows, 2 * cw), kind),
            pltpu.VMEM((2, 2, nd, nz, rows, 2 * cw), kind),
            pltpu.VMEM((2, 2, 2, 2, rr, cw), kind),
            pltpu.VMEM((steps, 2, nz, 2, rr, cw), kind),
            pltpu.VMEM((steps, 2, 2, nz, rr, cw), kind),
            pltpu.VMEM((steps, 2, nz, rr, cw), F32),
            pltpu.VMEM((steps, 2, nz, rr, cw), F32),
            pltpu.VMEM((steps, 2, nz, rr, cw), F32),
            pltpu.VMEM((steps, 2, nz, rr, cw), F32),
            pltpu.VMEM((2, steps, nz, rr, cw), F32),
            pltpu.VMEM((2, steps, nz, rr, cw), F32),
            pltpu.VMEM((2, steps, nz, rr, cw), F32),
            pltpu.VMEM((2, steps, nz, rr, cw), F32),
            pltpu.VMEM((2, nz - 1, 2, 2, 2, rr, cw), kind),
            pltpu.VMEM((2, 2, 2, rr, cw), F32),
            pltpu.VMEM((2, 2, 2, rr, cw), F32),
            pltpu.VMEM((2, 2, 2, rr, cw), F32),
            pltpu.VMEM((2, 3, rr, cw), F32),
            pltpu.VMEM((nd, rows, width), F32),
            pltpu.VMEM((rows, width), F32),
            pltpu.VMEM((rows, width), F32),
            pltpu.VMEM((nd, edge, width), F32),
            pltpu.VMEM((nd, edge, width), F32),
            dma((4,)),
            dma((2, steps)), dma((2, steps)),
            dma((2, steps)), dma((2, steps)),
            dma((2, steps)), dma((2, steps)),
            dma((2, steps, nz - 1)), dma((2, steps, nz - 1)),
            dma((2, nz - 1)), dma((2, nz - 1)),
            dma((2,)), dma((2,)),
            dma((2, 3)), dma((2, 3)),
            dma((4, 2, steps + 1)), dma((4, 2, steps + 1)),
        ],
        compiler_params=pltpu.CompilerParams(collective_id=0, has_side_effects=True),
    )(src)


def solution(mesh):
    groups, members = mesh.shape["shot"], mesh.shape["tile"]
    return jax.shard_map(
        functools.partial(body, groups, members),
        mesh=mesh,
        in_specs=(P(("shot", "tile"), None, None, None),),
        out_specs=P("shot", "tile", None),
        check_vma=False,
    )
```

```python
import functools

import jax
import jax.numpy as jnp
from jax import lax
from jax.experimental import pallas as pl
from jax.experimental.pallas import tpu as pltpu
from jax.sharding import PartitionSpec as P

MESH = pl.DeviceIdType.MESH
F32 = jnp.float32


def kernel(groups, members, src, out, own_a, own_b, own_c, r1a, r1b, s1a, s1b, r2a, r2b,
           s2, r3, s3, r4, rz, sc, rc, tc, rd, img, low, high, top, bottom, own_sem,
           p1s, p1r, q1s, q1r, p2s, p2r, p3s, p3r, zs, zr, cs, cr, ds, dr, hs, hr):
    nd, nz, rows, width = src.shape[2], src.shape[3], src.shape[5], src.shape[6]
    cw = width // 4
    rr = s2.shape[3]
    parts = rows // rr
    edge = top.shape[1]
    units = [(j, d, h * rr) for j in range(2) for d in range(nd) for h in range(parts)]
    crows = own_c.shape[4]
    c_unit = (1, nd - 1, rows - crows)
    cj, cd, ch = c_unit
    units = units[: len(units) - crows // rr]
    steps = len(units)
    g, t = lax.axis_index("shot"), lax.axis_index("tile")
    x, c = g // 2, g % 2
    z, y = t // 2, t % 2

    def dev(gx, tx):
        return {"shot": gx, "tile": tx}

    x_peer = dev((1 - x) * 2 + c, t)
    c_peer = dev(x * 2 + 1 - c, t)
    y_peer = dev(g, z * 2 + 1 - y)
    d_peer = dev((1 - x) * 2 + c, z * 2 + 1 - y)

    def z_peer(o):
        return dev(g, lax.rem(z + o, nz) * 2 + y)

    beside = [
        (g > 0, dev(g - 1, t)),
        (g < groups - 1, dev(g + 1, t)),
        (t > 0, dev(g, t - 1)),
        (t < members - 1, dev(g, t + 1)),
    ]

    def col(kind, j):
        return pl.ds((2 * kind + j) * cw, cw)

    def row(h):
        return pl.ds(h, rr)

    c_row = pl.ds(ch, crows)

    barrier = pltpu.get_barrier_semaphore()
    peers = [x_peer, c_peer, y_peer, d_peer] + [z_peer(o) for o in range(1, nz)]
    count = jnp.int32(len(peers))
    for peer in peers:
        pl.semaphore_signal(barrier, inc=1, device_id=peer, device_id_type=MESH)
    for there, peer in beside:
        count = count + jnp.where(there, 1, 0)

        @pl.when(there)
        def _():
            pl.semaphore_signal(barrier, inc=1, device_id=peer, device_id_type=MESH)
    loads = [
        pltpu.make_async_copy(src.at[x, :, :, :, :, :, pl.ds(0, 2 * cw)], own_a, own_sem.at[0]),
        pltpu.make_async_copy(src.at[:, :, :, :, y, :, pl.ds(2 * cw, 2 * cw)], own_b, own_sem.at[1]),
    ]
    for kind in range(2):
        loads.append(pltpu.make_async_copy(src.at[:, :, cd, z, :, c_row, col(kind, cj)],
                                           own_c.at[kind], own_sem.at[2 + kind]))
    for copy in loads:
        copy.start()
    pl.semaphore_wait(barrier, count)

    def remote(a, b, s, r, peer):
        copy = pltpu.make_async_remote_copy(
            src_ref=a, dst_ref=b, send_sem=s, recv_sem=r, device_id=peer, device_id_type=MESH
        )
        copy.start()
        return copy

    def done(ref, sem):
        pltpu.make_async_copy(ref, ref, sem).wait()

    first, second, third, fourth = {}, {}, {}, {}

    def p1(k):
        j, d, h = units[k]
        first[k] = (
            remote(src.at[1 - x, :, d, :, :, row(h), col(0, j)], r1a.at[k],
                   p1s.at[0], p1r.at[0, k], x_peer),
            remote(src.at[:, :, d, :, 1 - y, row(h), col(1, j)], r1b.at[k],
                   p1s.at[1], p1r.at[1, k], y_peer),
        )

    def two_a(k, core, side):
        j, d, h = units[k]
        own = own_a[core, d, :, side, row(h), pl.ds(j * cw, cw)]
        return own.astype(F32) + r1a[k, core, :, side].astype(F32)

    def two_b(k, core, side):
        j, d, h = units[k]
        own = own_b[side, core, d, :, row(h), pl.ds(j * cw, cw)]
        return own.astype(F32) + r1b[k, side, core].astype(F32)

    def q1(k):
        a, b = first[k]
        a.wait_recv()
        for side in range(2):
            s1a[k, side] = two_a(k, 1 - c, side)
        ca = remote(s1a.at[k], r2a.at[k], q1s.at[0], q1r.at[0, k], c_peer)
        b.wait_recv()
        for side in range(2):
            s1b[k, side] = two_b(k, 1 - c, side)
        cb = remote(s1b.at[k], r2b.at[k], q1s.at[1], q1r.at[1, k], c_peer)
        second[k] = (ca, cb)

    def p2(k):
        a, b = second[k]
        a.wait_recv()
        s2[0, k] = two_a(k, c, 1 - y) + r2a[k, 1 - y]
        ca = remote(s2.at[0, k], r3.at[0, k], p2s.at[0], p2r.at[0, k], y_peer)
        b.wait_recv()
        s2[1, k] = two_b(k, c, 1 - x) + r2b[k, 1 - x]
        cb = remote(s2.at[1, k], r3.at[1, k], p2s.at[1], p2r.at[1, k], x_peer)
        third[k] = (ca, cb)

    def p3(k):
        copies = []
        for kind in range(2):
            third[k][kind].wait_recv()
            if kind == 0:
                s3[0, k] = two_a(k, c, y) + r2a[k, y] + r3[0, k]
            else:
                s3[1, k] = two_b(k, c, x) + r2b[k, x] + r3[1, k]
            for o in range(1, nz):
                to = lax.rem(z + o, nz)
                copies.append(remote(s3.at[kind, k, to], r4.at[kind, k, z],
                                     p3s.at[kind], p3r.at[kind, k], z_peer(o)))
        fourth[k] = copies

    z_first, z_core, z_last = [], [], []

    def c_z():
        for kind in range(2):
            for o in range(1, nz):
                to = lax.rem(z + o, nz)
                z_first.append(remote(src.at[:, :, cd, to, :, c_row, col(kind, cj)], rz.at[kind, o - 1],
                                      zs.at[kind], zr.at[kind], z_peer(o)))

    def c_sum(kind, core, side):
        total = own_c[kind, side, core].astype(F32)
        for o in range(1, nz):
            total = total + rz[kind, o - 1, side, core].astype(F32)
        return total

    def c_core():
        for kind in range(2):
            done(rz.at[kind], zr.at[kind])
            for side in range(2):
                sc[kind, side] = c_sum(kind, 1 - c, side)
            z_core.append(remote(sc.at[kind], rc.at[kind], cs.at[kind], cr.at[kind], c_peer))

    def c_xy():
        for kind in range(2):
            z_core[kind].wait_recv()
            for side in range(2):
                tc[kind, side] = c_sum(kind, c, side) + rc[kind, side]
            for i, (a, b, peer) in enumerate(
                [(1 - x, 1 - y, d_peer), (1 - x, y, x_peer), (x, 1 - y, y_peer)]
            ):
                z_last.append(remote(tc.at[kind, a, b], rd.at[kind, i], ds.at[kind], dr.at[kind], peer))

    scale = 1.0 / jnp.sqrt(F32(groups * members))

    def halo(side, a, b):
        there, peer = beside[side]

        @pl.when(there)
        def _():
            remote(a, b, hs.at[side], hr.at[side], peer)

    def finish(kind, unit, total):
        j, d, h = unit
        cols = col(kind, j)
        span = pl.ds(h, total.shape[0])
        img[d, span, cols] = total * scale
        if d == 0:
            halo(0, img.at[d, span, cols], high.at[span, cols])
        if d == nd - 1:
            halo(1, img.at[d, span, cols], low.at[span, cols])
        if h == 0:
            halo(2, img.at[d, pl.ds(0, edge), cols], bottom.at[d, :, cols])
        if h + total.shape[0] == rows:
            halo(3, img.at[d, pl.ds(rows - edge, edge), cols], top.at[d, :, cols])

    def last(k):
        for kind in range(2):
            total = s3[kind, k, z]
            done(r4.at[kind, k, pl.ds(0, nz - 1)], p3r.at[kind, k])
            for o in range(1, nz):
                total = total + r4[kind, k, lax.rem(z + nz - o, nz)]
            finish(kind, units[k], total)

    def c_last():
        for kind in range(2):
            total = tc[kind, x, y]
            done(rd.at[kind], dr.at[kind])
            for i in range(3):
                total = total + rd[kind, i]
            finish(kind, c_unit, total)

    ahead, lag2, lag3, lag4 = 3, 0, 2, 4
    at_core = min(3, steps - 1)
    at_xy = max(steps - 2, at_core)
    p1(0)
    c_z()
    for k in range(1, min(ahead, steps)):
        p1(k)
    for copy in loads:
        copy.wait()
    for k in range(steps + lag4):
        if k < steps:
            q1(k)
        if 0 <= k - lag2 < steps:
            p2(k - lag2)
        if k + ahead < steps:
            p1(k + ahead)
        if 0 <= k - lag3 < steps:
            p3(k - lag3)
        if k == at_core:
            c_core()
        if k == at_xy:
            c_xy()
        if k == steps + lag4 - 1:
            c_last()
        if 0 <= k - lag4 < steps:
            last(k - lag4)
    for side, ref in enumerate([high, low, bottom, top]):
        @pl.when(beside[side ^ 1][0])
        def _():
            done(ref, hr.at[side])

    rown = lax.broadcasted_iota(jnp.int32, (rows, width), 0)
    coln = lax.broadcasted_iota(jnp.int32, (rows, width), 1)
    for d in range(nd):
        here = img[d]
        below = img[d - 1] if d > 0 else jnp.where(g > 0, low[...], 0.0)
        above = img[d + 1] if d < nd - 1 else jnp.where(g < groups - 1, high[...], 0.0)
        before = jnp.where(t > 0, top[d, edge - 1:edge, :], 0.0)
        after = jnp.where(t < members - 1, bottom[d, 0:1, :], 0.0)
        near = above + below
        near = near + jnp.where(rown == rows - 1, after, pltpu.roll(here, rows - 1, 0))
        near = near + jnp.where(rown == 0, before, pltpu.roll(here, 1, 0))
        near = near + jnp.where(coln == width - 1, 0.0, pltpu.roll(here, width - 1, 1))
        near = near + jnp.where(coln == 0, 0.0, pltpu.roll(here, 1, 1))
        out[d] = 6.0 * here - near
    for side, ref in enumerate([high, low, bottom, top]):
        @pl.when(beside[side][0])
        def _():
            done(ref, hs.at[side])
    for kind, (one, two) in enumerate([(r1a, r2a), (r1b, r2b)]):
        done(one, p1s.at[kind])
        done(two, q1s.at[kind])
        done(r3.at[kind], p2s.at[kind])
        done(r4.at[kind, :, pl.ds(0, nz - 1)], p3s.at[kind])
        done(rz.at[kind], zs.at[kind])
        done(rc.at[kind], cs.at[kind])
        done(rd.at[kind], ds.at[kind])


def body(groups, members, partials):
    shots, depth, lateral, width = partials.shape
    nd, nz, rows, cw = depth // groups, members // 2, lateral // members, width // 4
    parts = 2 if rows % 32 == 0 else 1
    rr, edge = rows // parts, min(8, rows)
    crows = rr
    steps = 2 * nd * parts - crows // rr
    src = partials.reshape(2, 2, nd, nz, 2, rows, width)
    kind = partials.dtype
    dma = pltpu.SemaphoreType.DMA
    return pl.pallas_call(
        functools.partial(kernel, groups, members),
        out_shape=jax.ShapeDtypeStruct((nd, rows, width), F32),
        in_specs=[pl.BlockSpec(memory_space=pl.ANY)],
        out_specs=pl.BlockSpec(memory_space=pltpu.VMEM),
        scratch_shapes=[
            pltpu.VMEM((2, nd, nz, 2, rows, 2 * cw), kind),
            pltpu.VMEM((2, 2, nd, nz, rows, 2 * cw), kind),
            pltpu.VMEM((2, 2, 2, 2, crows, cw), kind),
            pltpu.VMEM((steps, 2, nz, 2, rr, cw), kind),
            pltpu.VMEM((steps, 2, 2, nz, rr, cw), kind),
            pltpu.VMEM((steps, 2, nz, rr, cw), F32),
            pltpu.VMEM((steps, 2, nz, rr, cw), F32),
            pltpu.VMEM((steps, 2, nz, rr, cw), F32),
            pltpu.VMEM((steps, 2, nz, rr, cw), F32),
            pltpu.VMEM((2, steps, nz, rr, cw), F32),
            pltpu.VMEM((2, steps, nz, rr, cw), F32),
            pltpu.VMEM((2, steps, nz, rr, cw), F32),
            pltpu.VMEM((2, steps, nz, rr, cw), F32),
            pltpu.VMEM((2, nz - 1, 2, 2, 2, crows, cw), kind),
            pltpu.VMEM((2, 2, 2, crows, cw), F32),
            pltpu.VMEM((2, 2, 2, crows, cw), F32),
            pltpu.VMEM((2, 2, 2, crows, cw), F32),
            pltpu.VMEM((2, 3, crows, cw), F32),
            pltpu.VMEM((nd, rows, width), F32),
            pltpu.VMEM((rows, width), F32),
            pltpu.VMEM((rows, width), F32),
            pltpu.VMEM((nd, edge, width), F32),
            pltpu.VMEM((nd, edge, width), F32),
            dma((4,)),
            dma((2,)), dma((2, steps)),
            dma((2,)), dma((2, steps)),
            dma((2,)), dma((2, steps)),
            dma((2,)), dma((2, steps)),
            dma((2,)), dma((2,)),
            dma((2,)), dma((2,)),
            dma((2,)), dma((2,)),
            dma((4,)), dma((4,)),
        ],
        compiler_params=pltpu.CompilerParams(collective_id=0, has_side_effects=True),
    )(src)


def solution(mesh):
    groups, members = mesh.shape["shot"], mesh.shape["tile"]
    return jax.shard_map(
        functools.partial(body, groups, members),
        mesh=mesh,
        in_specs=(P(("shot", "tile"), None, None, None),),
        out_specs=P("shot", "tile", None),
        check_vma=False,
    )
```

```python
import functools

import jax
import jax.numpy as jnp
from jax import lax
from jax.experimental import pallas as pl
from jax.experimental.pallas import tpu as pltpu
from jax.sharding import PartitionSpec as P

MESH = pl.DeviceIdType.MESH
F32 = jnp.float32


def kernel(groups, members, src, out, own_a, own_b, own_c, r1a, r1b, s1a, s1b, r2a, r2b,
           s2, r3, s3, r4, rz, sc, rc, tc, rd, img, low, high, top, bottom, own_sem,
           p1s, p1r, q1s, q1r, p2s, p2r, p3s, p3r, zs, zr, cs, cr, ds, dr, hs, hr):
    nd, nz, rows, width = src.shape[2], src.shape[3], src.shape[5], src.shape[6]
    cw = width // 4
    rr = s2.shape[3]
    parts = rows // rr
    edge = top.shape[1]
    units = [(j, d, h * rr) for j in range(2) for d in range(nd) for h in range(parts)]
    crows = own_c.shape[4]
    c_unit = (1, nd - 1, rows - crows)
    cj, cd, ch = c_unit
    units = units[: len(units) - crows // rr]
    steps = len(units)
    g, t = lax.axis_index("shot"), lax.axis_index("tile")
    x, c = g // 2, g % 2
    z, y = t // 2, t % 2

    def dev(gx, tx):
        return {"shot": gx, "tile": tx}

    x_peer = dev((1 - x) * 2 + c, t)
    c_peer = dev(x * 2 + 1 - c, t)
    y_peer = dev(g, z * 2 + 1 - y)
    d_peer = dev((1 - x) * 2 + c, z * 2 + 1 - y)

    def z_peer(o):
        return dev(g, lax.rem(z + o, nz) * 2 + y)

    beside = [
        (g > 0, dev(g - 1, t)),
        (g < groups - 1, dev(g + 1, t)),
        (t > 0, dev(g, t - 1)),
        (t < members - 1, dev(g, t + 1)),
    ]

    def col(kind, j):
        return pl.ds((2 * kind + j) * cw, cw)

    def row(h):
        return pl.ds(h, rr)

    c_row = pl.ds(ch, crows)

    barrier = pltpu.get_barrier_semaphore()
    peers = [x_peer, c_peer, y_peer, d_peer] + [z_peer(o) for o in range(1, nz)]
    count = jnp.int32(len(peers))
    for peer in peers:
        pl.semaphore_signal(barrier, inc=1, device_id=peer, device_id_type=MESH)
    for there, peer in beside:
        count = count + jnp.where(there, 1, 0)

        @pl.when(there)
        def _():
            pl.semaphore_signal(barrier, inc=1, device_id=peer, device_id_type=MESH)
    loads = [
        pltpu.make_async_copy(src.at[x, :, :, :, :, :, pl.ds(0, 2 * cw)], own_a, own_sem.at[0]),
        pltpu.make_async_copy(src.at[:, :, :, :, y, :, pl.ds(2 * cw, 2 * cw)], own_b, own_sem.at[1]),
    ]
    for kind in range(2):
        loads.append(pltpu.make_async_copy(src.at[:, :, cd, z, :, c_row, col(kind, cj)],
                                           own_c.at[kind], own_sem.at[2 + kind]))
    for copy in loads:
        copy.start()
    pl.semaphore_wait(barrier, count)

    def remote(a, b, s, r, peer):
        copy = pltpu.make_async_remote_copy(
            src_ref=a, dst_ref=b, send_sem=s, recv_sem=r, device_id=peer, device_id_type=MESH
        )
        copy.start()
        return copy

    def done(ref, sem):
        pltpu.make_async_copy(ref, ref, sem).wait()

    first, second, third, fourth = {}, {}, {}, {}

    def p1(k):
        j, d, h = units[k]
        first[k] = (
            remote(src.at[1 - x, :, d, :, :, row(h), col(0, j)], r1a.at[k],
                   p1s.at[0], p1r.at[0, k], x_peer),
            remote(src.at[:, :, d, :, 1 - y, row(h), col(1, j)], r1b.at[k],
                   p1s.at[1], p1r.at[1, k], y_peer),
        )

    def two_a(k, core, side):
        j, d, h = units[k]
        own = own_a[core, d, :, side, row(h), pl.ds(j * cw, cw)]
        return own.astype(F32) + r1a[k, core, :, side].astype(F32)

    def two_b(k, core, side):
        j, d, h = units[k]
        own = own_b[side, core, d, :, row(h), pl.ds(j * cw, cw)]
        return own.astype(F32) + r1b[k, side, core].astype(F32)

    def q1(k):
        a, b = first[k]
        a.wait_recv()
        for side in range(2):
            s1a[k, side] = two_a(k, 1 - c, side)
        ca = remote(s1a.at[k], r2a.at[k], q1s.at[0], q1r.at[0, k], c_peer)
        b.wait_recv()
        for side in range(2):
            s1b[k, side] = two_b(k, 1 - c, side)
        cb = remote(s1b.at[k], r2b.at[k], q1s.at[1], q1r.at[1, k], c_peer)
        second[k] = (ca, cb)

    def p2(k):
        a, b = second[k]
        a.wait_recv()
        s2[0, k] = two_a(k, c, 1 - y) + r2a[k, 1 - y]
        ca = remote(s2.at[0, k], r3.at[0, k], p2s.at[0], p2r.at[0, k], y_peer)
        b.wait_recv()
        s2[1, k] = two_b(k, c, 1 - x) + r2b[k, 1 - x]
        cb = remote(s2.at[1, k], r3.at[1, k], p2s.at[1], p2r.at[1, k], x_peer)
        third[k] = (ca, cb)

    def p3(k):
        copies = []
        for kind in range(2):
            third[k][kind].wait_recv()
            if kind == 0:
                s3[0, k] = two_a(k, c, y) + r2a[k, y] + r3[0, k]
            else:
                s3[1, k] = two_b(k, c, x) + r2b[k, x] + r3[1, k]
            for o in range(1, nz):
                to = lax.rem(z + o, nz)
                copies.append(remote(s3.at[kind, k, to], r4.at[kind, k, z],
                                     p3s.at[kind], p3r.at[kind, k], z_peer(o)))
        fourth[k] = copies

    z_first, z_core, z_last = [], [], []

    def c_z():
        for kind in range(2):
            for o in range(1, nz):
                to = lax.rem(z + o, nz)
                z_first.append(remote(src.at[:, :, cd, to, :, c_row, col(kind, cj)], rz.at[kind, o - 1],
                                      zs.at[kind], zr.at[kind], z_peer(o)))

    def c_sum(kind, core, side):
        total = own_c[kind, side, core].astype(F32)
        for o in range(1, nz):
            total = total + rz[kind, o - 1, side, core].astype(F32)
        return total

    def c_core():
        for kind in range(2):
            done(rz.at[kind], zr.at[kind])
            for side in range(2):
                sc[kind, side] = c_sum(kind, 1 - c, side)
            z_core.append(remote(sc.at[kind], rc.at[kind], cs.at[kind], cr.at[kind], c_peer))

    def c_xy():
        for kind in range(2):
            z_core[kind].wait_recv()
            for side in range(2):
                tc[kind, side] = c_sum(kind, c, side) + rc[kind, side]
            for i, (a, b, peer) in enumerate(
                [(1 - x, 1 - y, d_peer), (1 - x, y, x_peer), (x, 1 - y, y_peer)]
            ):
                z_last.append(remote(tc.at[kind, a, b], rd.at[kind, i], ds.at[kind], dr.at[kind], peer))

    scale = 1.0 / jnp.sqrt(F32(groups * members))

    def halo(side, a, b):
        there, peer = beside[side]

        @pl.when(there)
        def _():
            remote(a, b, hs.at[side], hr.at[side], peer)

    def finish(kind, unit, total):
        j, d, h = unit
        cols = col(kind, j)
        span = pl.ds(h, total.shape[0])
        img[d, span, cols] = total * scale
        if d == 0:
            halo(0, img.at[d, span, cols], high.at[span, cols])
        if d == nd - 1:
            halo(1, img.at[d, span, cols], low.at[span, cols])
        if h == 0:
            halo(2, img.at[d, pl.ds(0, edge), cols], bottom.at[d, :, cols])
        if h + total.shape[0] == rows:
            halo(3, img.at[d, pl.ds(rows - edge, edge), cols], top.at[d, :, cols])

    def last(k):
        for kind in range(2):
            total = s3[kind, k, z]
            done(r4.at[kind, k, pl.ds(0, nz - 1)], p3r.at[kind, k])
            for o in range(1, nz):
                total = total + r4[kind, k, lax.rem(z + nz - o, nz)]
            finish(kind, units[k], total)

    def c_last():
        for kind in range(2):
            total = tc[kind, x, y]
            done(rd.at[kind], dr.at[kind])
            for i in range(3):
                total = total + rd[kind, i]
            finish(kind, c_unit, total)

    ahead, lag2, lag3, lag4 = 3, 0, 3, 7
    at_core = min(6, steps - 1)
    at_xy = max(steps - 2, at_core)
    p1(0)
    c_z()
    for k in range(1, min(ahead, steps)):
        p1(k)
    for copy in loads:
        copy.wait()
    for k in range(steps + lag4):
        if k < steps:
            q1(k)
        if 0 <= k - lag2 < steps:
            p2(k - lag2)
        if k + ahead < steps:
            p1(k + ahead)
        if 0 <= k - lag3 < steps:
            p3(k - lag3)
        if k == at_core:
            c_core()
        if k == at_xy:
            c_xy()
        if k == steps + lag4 - 1:
            c_last()
        if 0 <= k - lag4 < steps:
            last(k - lag4)
    for side, ref in enumerate([high, low, bottom, top]):
        @pl.when(beside[side ^ 1][0])
        def _():
            done(ref, hr.at[side])

    rown = lax.broadcasted_iota(jnp.int32, (rows, width), 0)
    coln = lax.broadcasted_iota(jnp.int32, (rows, width), 1)
    for d in range(nd):
        here = img[d]
        below = img[d - 1] if d > 0 else jnp.where(g > 0, low[...], 0.0)
        above = img[d + 1] if d < nd - 1 else jnp.where(g < groups - 1, high[...], 0.0)
        before = jnp.where(t > 0, top[d, edge - 1:edge, :], 0.0)
        after = jnp.where(t < members - 1, bottom[d, 0:1, :], 0.0)
        near = above + below
        near = near + jnp.where(rown == rows - 1, after, pltpu.roll(here, rows - 1, 0))
        near = near + jnp.where(rown == 0, before, pltpu.roll(here, 1, 0))
        near = near + jnp.where(coln == width - 1, 0.0, pltpu.roll(here, width - 1, 1))
        near = near + jnp.where(coln == 0, 0.0, pltpu.roll(here, 1, 1))
        out[d] = 6.0 * here - near
    for side, ref in enumerate([high, low, bottom, top]):
        @pl.when(beside[side][0])
        def _():
            done(ref, hs.at[side])
    for kind, (one, two) in enumerate([(r1a, r2a), (r1b, r2b)]):
        done(one, p1s.at[kind])
        done(two, q1s.at[kind])
        done(r3.at[kind], p2s.at[kind])
        done(r4.at[kind, :, pl.ds(0, nz - 1)], p3s.at[kind])
        done(rz.at[kind], zs.at[kind])
        done(rc.at[kind], cs.at[kind])
        done(rd.at[kind], ds.at[kind])


def body(groups, members, partials):
    shots, depth, lateral, width = partials.shape
    nd, nz, rows, cw = depth // groups, members // 2, lateral // members, width // 4
    parts = 4 if rows % 64 == 0 else 1
    rr, edge = rows // parts, min(8, rows)
    crows = 2 * rr if parts > 1 else rr
    steps = 2 * nd * parts - crows // rr
    src = partials.reshape(2, 2, nd, nz, 2, rows, width)
    kind = partials.dtype
    dma = pltpu.SemaphoreType.DMA
    return pl.pallas_call(
        functools.partial(kernel, groups, members),
        out_shape=jax.ShapeDtypeStruct((nd, rows, width), F32),
        in_specs=[pl.BlockSpec(memory_space=pl.ANY)],
        out_specs=pl.BlockSpec(memory_space=pltpu.VMEM),
        scratch_shapes=[
            pltpu.VMEM((2, nd, nz, 2, rows, 2 * cw), kind),
            pltpu.VMEM((2, 2, nd, nz, rows, 2 * cw), kind),
            pltpu.VMEM((2, 2, 2, 2, crows, cw), kind),
            pltpu.VMEM((steps, 2, nz, 2, rr, cw), kind),
            pltpu.VMEM((steps, 2, 2, nz, rr, cw), kind),
            pltpu.VMEM((steps, 2, nz, rr, cw), F32),
            pltpu.VMEM((steps, 2, nz, rr, cw), F32),
            pltpu.VMEM((steps, 2, nz, rr, cw), F32),
            pltpu.VMEM((steps, 2, nz, rr, cw), F32),
            pltpu.VMEM((2, steps, nz, rr, cw), F32),
            pltpu.VMEM((2, steps, nz, rr, cw), F32),
            pltpu.VMEM((2, steps, nz, rr, cw), F32),
            pltpu.VMEM((2, steps, nz, rr, cw), F32),
            pltpu.VMEM((2, nz - 1, 2, 2, 2, crows, cw), kind),
            pltpu.VMEM((2, 2, 2, crows, cw), F32),
            pltpu.VMEM((2, 2, 2, crows, cw), F32),
            pltpu.VMEM((2, 2, 2, crows, cw), F32),
            pltpu.VMEM((2, 3, crows, cw), F32),
            pltpu.VMEM((nd, rows, width), F32),
            pltpu.VMEM((rows, width), F32),
            pltpu.VMEM((rows, width), F32),
            pltpu.VMEM((nd, edge, width), F32),
            pltpu.VMEM((nd, edge, width), F32),
            dma((4,)),
            dma((2,)), dma((2, steps)),
            dma((2,)), dma((2, steps)),
            dma((2,)), dma((2, steps)),
            dma((2,)), dma((2, steps)),
            dma((2,)), dma((2,)),
            dma((2,)), dma((2,)),
            dma((2,)), dma((2,)),
            dma((4,)), dma((4,)),
        ],
        compiler_params=pltpu.CompilerParams(collective_id=0, has_side_effects=True),
    )(src)


def solution(mesh):
    groups, members = mesh.shape["shot"], mesh.shape["tile"]
    return jax.shard_map(
        functools.partial(body, groups, members),
        mesh=mesh,
        in_specs=(P(("shot", "tile"), None, None, None),),
        out_specs=P("shot", "tile", None),
        check_vma=False,
    )
```
